32 devices in a mesh: dp: 8 (over y, x, core), tensor: 4 (over z).
Axes of the slice: x: 2, y: 2, z: 4, core: 2. Of those that a mesh axis runs over, the one named last changes fastest.
Arguments:
- activations: bfloat16 [1, 1024, 4096], P(None, ('dp', 'tensor')), may hold values from -6 to 6
- out_grad: bfloat16 [1, 1024, 512], P(None, 'dp', 'tensor'), may hold values from -0.5 to 0.5
- value_weight: bfloat16 [1, 512, 4096], P(None, 'tensor'), may hold values from -6 to 6
- error_feedback: bfloat16 [1, 8, 512, 4096], P(None, 'dp', 'tensor'), may hold values from -8 to 8
- warm_right: bfloat16 [1, 4, 4096, 32], P(None, 'tensor'), may hold values from -6 to 6
Outputs:
- new_error: bfloat16 [1, 8, 512, 4096], P(None, 'dp', 'tensor')
- left_basis: float32 [1, 512, 32], P(None, 'tensor')
- right_factor: bfloat16 [1, 4, 4096, 32], P(None, 'tensor')
- input_grad: bfloat16 [1, 1024, 4096], P(None, ('dp', 'tensor'))
The draws below stay inside these ranges and needn't reach their ends.
All inputs are finite; a program needn't handle non-finite values.
Results may differ from the reference program's by a relative error of at most 0.00065.
Values may be sent and summed in bfloat16 or wider, within the bound.
A program may use at most 64 MiB of HBM per device.

```python
import jax
import jax.numpy as jnp
from jax import lax

D = 4096
HEAD = 128
R = 32
LAYERS = 1
VALUE_HEADS = 4
VALUE_WIDTH = 512
REP_TOK = 128
TOKENS = 1024
N_DP = 8


def draw_error_feedback(key, part):
    shared_key = jax.random.fold_in(key, 11)
    own_key = jax.random.fold_in(key, 12)
    shared = jax.random.normal(shared_key, (LAYERS, 1, VALUE_WIDTH, D), jnp.float32)
    own = jax.random.normal(own_key, (LAYERS, N_DP, VALUE_WIDTH, D), jnp.float32)
    values = shared + 0.5 * own
    return jnp.clip(values, -8.0, 8.0).astype(jnp.bfloat16)


def block_scale(rng, dims, shards, low, high):
    def one(position, parts):
        steps = jax.random.uniform(jax.random.fold_in(jax.random.fold_in(rng, 6), position), (parts,), jnp.float32, low / len(shards), high / len(shards))
        return jnp.repeat(jnp.exp(steps), dims[position] // parts).reshape((-1,) + (1,) * (len(dims) - position - 1))

    level = one(*shards[0])
    for cut in shards[1:]:
        level = level * one(*cut)
    return level


def scatter_about(stream_key, shape, width, limit, pieces=(), dtype=jnp.bfloat16):
    entries = width * jax.random.normal(stream_key, shape, jnp.float32)
    if pieces:
        entries = entries * block_scale(stream_key, shape, pieces, -0.22, 0.18)
    return jnp.clip(entries, -limit, limit).astype(dtype)


def setup_inputs(seed: int = 0) -> dict:
    arg_keys = jax.random.split(jax.random.key(seed), 6)
    activations = scatter_about(arg_keys[0], (LAYERS, TOKENS, D), 1.0, 6.0, ((1, 32),))
    out_grad = scatter_about(arg_keys[1], (LAYERS, TOKENS, VALUE_WIDTH), REP_TOK ** -0.5, 0.5, ((1, 8), (2, 4)))
    value_weight = scatter_about(arg_keys[2], (LAYERS, VALUE_WIDTH, D), 1.0, 6.0, ((1, 4),))
    error_feedback = draw_error_feedback(jax.random.fold_in(arg_keys[5], 71), 0)
    warm_right = scatter_about(arg_keys[4], (LAYERS, VALUE_HEADS, D, R), 1.0, 6.0, ((1, 4),))
    return dict(activations=activations, out_grad=out_grad, value_weight=value_weight, error_feedback=error_feedback, warm_right=warm_right)


HIGH = lax.Precision.HIGHEST

def orthonormal(left):
    gram = jnp.einsum('bhk,bhj->bkj', left, left, precision=HIGH)
    lower = jnp.linalg.cholesky(gram)
    return lax.linalg.triangular_solve(lower, left, left_side=False, lower=True, transpose_a=True)

def reference(activations, out_grad, value_weight, error_feedback, warm_right):
    errors = []
    bases = []
    rights = []
    inputs = []
    for layer in range(LAYERS):
        tokens = activations[layer].reshape(N_DP, REP_TOK, D).astype(jnp.float32)
        grads = out_grad[layer].reshape(N_DP, REP_TOK, VALUE_WIDTH).astype(jnp.float32)
        weight_grad = jnp.einsum('rtk,rtd->rkd', grads, tokens, precision=HIGH)
        merged = weight_grad + error_feedback[layer].astype(jnp.float32)
        blocks = merged.reshape(N_DP, VALUE_HEADS, HEAD, D)
        warm = warm_right[layer].astype(jnp.float32)
        left = jnp.einsum('rbhd,bdk->bhk', blocks, warm, precision=HIGH) / N_DP
        basis = orthonormal(left)
        right = jnp.einsum('rbhd,bhk->bdk', blocks, basis, precision=HIGH) / N_DP
        approx = jnp.einsum('bhk,bdk->bhd', basis, right, precision=HIGH)
        residual = (blocks - approx[None]).reshape(N_DP, VALUE_WIDTH, D)
        errors.append(residual.astype(jnp.bfloat16))
        bases.append(basis.reshape(VALUE_WIDTH, R))
        rights.append(right.astype(jnp.bfloat16))
        inputs.append(jnp.dot(out_grad[layer].astype(jnp.float32), value_weight[layer].astype(jnp.float32), preferred_element_type=jnp.float32).astype(jnp.bfloat16))
    return (jnp.stack(errors), jnp.stack(bases), jnp.stack(rights), jnp.stack(inputs))
```

```python
import functools

import jax
import jax.numpy as jnp
from jax import lax
from jax.experimental import pallas as pl
from jax.experimental.pallas import tpu as pltpu
from jax.sharding import PartitionSpec as P

MESH = pl.DeviceIdType.MESH
F32 = jnp.float32
BF16 = jnp.bfloat16
CHUNKS = 4
PIECES = 4


def split(x):
    high = x.astype(BF16)
    return high, (x - high.astype(F32)).astype(BF16)


def dot(a, b):
    return jnp.dot(a, b, preferred_element_type=F32)


def dot_nt(a, b):
    return lax.dot_general(a, b, (((1,), (1,)), ((), ())), preferred_element_type=F32)


def orthonormal(left, halfway):
    rank = left.shape[0]
    gram = lax.dot_general(
        left, left, (((1,), (1,)), ((), ())), precision=lax.Precision.HIGHEST, preferred_element_type=F32
    )
    row = lax.broadcasted_iota(jnp.int32, (rank, 1), 0)
    for k in range(rank):
        if k == rank // 2:
            halfway()
        scale = lax.rsqrt(gram[k : k + 1, k : k + 1])
        gram_row = gram[k : k + 1, :] * scale
        left_row = left[k : k + 1, :] * scale
        column = jnp.where(row > k, gram[:, k : k + 1] * scale, 0.0)
        gram = gram - column * gram_row
        left = jnp.where(row == k, left_row, left - column * left_row)
    return left


def kernel(
    ndp, nt, act_hbm, og_hbm, weight_hbm, error_hbm, warm_hbm,
    residual, basis_out, factor, input_grad,
    og, error, warm, loads, grad_sum, tokens, wall, oall, merged, lefts, part, halves, parts, right,
    act_send, act_recv, w_send, w_recv, f_send, f_recv, d_send, d_recv,
    o_send, o_recv, l_send, l_recv, h_send, h_recv, p_send, p_recv, r_send, r_recv, t_send,
):
    dp = lax.axis_index("dp")
    me = lax.axis_index("tensor")
    rows, width = act_hbm.shape
    head = og.shape[1]
    rank = warm.shape[0]
    spread = min(ndp, 8)
    slice_rows = head // spread
    cw = width // CHUNKS

    def copy(src, dst, send, recv, **device):
        return pltpu.make_async_remote_copy(
            src_ref=src, dst_ref=dst, send_sem=send, recv_sem=recv, device_id=device, device_id_type=MESH
        )

    def z_peer(o):
        return lax.rem(me + o, nt)

    def dp_peer(o):
        return lax.rem(dp + o, ndp)

    own_rows = pl.ds(pl.multiple_of(me * rows, rows), rows)
    loading = [
        pltpu.make_async_copy(src, dst, loads.at[i])
        for i, (src, dst) in enumerate((
            (act_hbm, tokens.at[own_rows, :]), (og_hbm, og), (weight_hbm, wall.at[me]),
            (error_hbm, error), (warm_hbm, warm),
        ))
    ]
    for load in loading:
        load.start()

    barrier = pltpu.get_barrier_semaphore()
    for o in range(1, nt):
        pl.semaphore_signal(barrier, inc=1, device_id={"tensor": z_peer(o)}, device_id_type=MESH)
    for o in range(1, ndp):
        pl.semaphore_signal(barrier, inc=1, device_id={"dp": dp_peer(o)}, device_id_type=MESH)
    pl.semaphore_wait(barrier, nt + ndp - 2)

    def token_block(b, c):
        return tokens.at[pl.ds(pl.multiple_of(b * rows, rows), rows), pl.ds(c * cw, cw)]

    own_slice = lax.rem(dp, spread)

    def weight_rows(s):
        return pl.ds(pl.multiple_of(s * slice_rows, slice_rows), slice_rows)

    def token_copy(b, c, way):
        return copy(
            token_block(b, c), token_block(b, c), act_send.at[way, b, c], act_recv.at[b, c],
            tensor=jnp.clip(me + (1 - 2 * way), 0, nt - 1),
        )

    def weight_copy(b, way):
        place = wall.at[b, weight_rows(own_slice), :]
        return copy(
            place, place, w_send.at[way, b], w_recv.at[b],
            tensor=jnp.clip(me + (1 - 2 * way), 0, nt - 1),
        )

    def has_next(way):
        return me < nt - 1 if way == 0 else me > 0

    def origin(way, s):
        b = me - s if way == 0 else me + s
        return b, (b >= 0 if way == 0 else b < nt), jnp.clip(b, 0, nt - 1)

    loading[0].wait()
    for c in range(CHUNKS):
        for way in range(2):
            @pl.when(has_next(way))
            def _():
                token_copy(me, c, way).start()
    loading[1].wait()
    for o in range(1, nt):
        q = z_peer(o)
        copy(
            og.at[pl.ds(pl.multiple_of(q * rows, rows), rows), :], oall.at[me], o_send.at[q], o_recv.at[me], tensor=q
        ).start()

    oall[me] = og[own_rows, :]
    og_t = og[...].astype(F32).T.astype(BF16)

    group = dp - own_slice
    core = lax.rem(dp, 2)
    chip = dp // 2
    partner = dp + 1 - 2 * core
    chips = spread // 2

    def slice_copy(b, s, q, send, recv):
        return copy(wall.at[b, weight_rows(s), :], wall.at[b, weight_rows(s), :], send, recv, dp=q)

    def chip_slice(o):
        return 2 * lax.rem(own_slice // 2 + o, chips) + core

    def chip_copy(b, o):
        s = chip_slice(o)
        return slice_copy(b, own_slice, group + s, f_send.at[b, s], f_recv.at[b, own_slice])

    def partner_copy(b, o):
        s = chip_slice(o)
        return slice_copy(b, s, partner, d_send.at[b, s], d_recv.at[b, s])

    def weight_relay(s):
        for way in range(2):
            _, valid, b = origin(way, s)

            @pl.when(valid)
            def _():
                weight_copy(b, way).wait_recv()

            @pl.when(jnp.logical_and(valid, has_next(way)))
            def _():
                weight_copy(b, way).start()

            @pl.when(valid)
            def _():
                for o in range(1, chips):
                    chip_copy(b, o).start()
                partner_copy(b, 0).start()

    def weight_partner(s):
        for way in range(2):
            _, valid, b = origin(way, s)

            @pl.when(valid)
            def _():
                for o in range(1, chips):
                    q = chip_slice(o)
                    slice_copy(b, q, group + q, f_send.at[b, q], f_recv.at[b, q]).wait_recv()
                    partner_copy(b, o).start()

    def add_input(b, first=False):
        for c in range(CHUNKS):
            cols = slice(c * cw, (c + 1) * cw)
            term = dot(oall[b], wall[b, :, cols])
            grad_sum[:, cols] = term if first else grad_sum[:, cols] + term

    def input_part(s):
        for way in range(2):
            _, valid, b = origin(way, s)

            @pl.when(valid)
            def _():
                copy(oall.at[b], oall.at[b], o_send.at[b], o_recv.at[b], tensor=b).wait_recv()
                for o in range(chips):
                    q = chip_slice(o) + 1 - 2 * core
                    slice_copy(b, q, partner, d_send.at[b, q], d_recv.at[b, q]).wait_recv()
                add_input(b)

    for load in loading[2:]:
        load.wait()
    add_input(me, True)

    left = jnp.zeros((rank, head), F32)
    for s in range(1, nt):
        for c in range(CHUNKS):
            for way in range(2):
                _, valid, b = origin(way, s)

                @pl.when(valid)
                def _():
                    token_copy(b, c, way).wait_recv()

                @pl.when(jnp.logical_and(valid, has_next(way)))
                def _():
                    token_copy(b, c, way).start()
            if s == nt - 1:
                cols = slice(c * cw, (c + 1) * cw)
                m = dot(og_t, tokens[:, cols]) + error[:, cols].astype(F32)
                merged[:, cols] = m
                high, low = split(m)
                w = warm[:, cols]
                left += dot_nt(w, high) + dot_nt(w, low)
        if s == 1:
            for way in range(2):
                @pl.when(has_next(way))
                def _():
                    weight_copy(me, way).start()
        elif s < nt - 1:
            weight_relay(s - 1)

    lefts[dp] = left
    for o in range(1, ndp):
        q = dp_peer(o)
        copy(lefts.at[dp], lefts.at[dp], l_send.at[q], l_recv.at[dp], dp=q).start()
    if nt > 2:
        weight_relay(nt - 2)

    for o in range(1, ndp):
        q = dp_peer(o)
        copy(lefts.at[q], lefts.at[q], l_send.at[q], l_recv.at[q], dp=q).wait_recv()
    total = lefts[0]
    for q in range(1, ndp):
        total += lefts[q]
    basis_t = orthonormal(total * (1.0 / ndp), lambda: weight_relay(nt - 1))
    basis = basis_t.T
    basis_out[...] = basis_t
    bt_high, bt_low = split(basis_t)
    bt_both = jnp.concatenate([bt_high, bt_low], axis=0)

    nchip = ndp // 2
    ncol = min(ndp, width // 128)
    nrow = ndp // ncol
    pw, ph = width // ncol, rank // nrow

    def piece(q_chip, q_core):
        p = q_core * nchip + q_chip
        r, c = p // ncol, lax.rem(p, ncol)
        return (
            pl.ds(pl.multiple_of(r * ph, ph), ph) if nrow > 1 else pl.ds(0, ph),
            pl.ds(pl.multiple_of(c * pw, pw), pw),
        )

    def chip_peer(o):
        return lax.rem(chip + o, nchip)

    def half_copy(i):
        return copy(part.at[piece(i, 1 - core)], halves.at[i], h_send.at[i], h_recv.at[i], dp=partner)

    def part_copy(q, slot):
        return copy(part.at[piece(q, core)], parts.at[slot], p_send.at[q], p_recv.at[slot], dp=2 * q + core)

    def compute_part(c):
        cols = pl.ds(pl.multiple_of(c * pw, pw), pw)
        high, low = split(merged[:, cols])
        both = dot(bt_both, high)
        part[:, cols] = both[:rank] + both[rank:] + dot(bt_high, low)

    if nrow == 1:
        for o in range(nchip):
            i = chip_peer(o + 1)
            compute_part((1 - core) * nchip + i)
            half_copy(i).start()
        for i in range(nchip):
            compute_part(core * nchip + i)
    else:
        for c in range(ncol):
            compute_part(c)
        for o in range(nchip):
            half_copy(chip_peer(o + 1)).start()
    for o in range(1, nchip):
        q = chip_peer(o)
        half_copy(q).wait_recv()
        part[piece(q, core)] += halves[q]
        part_copy(q, chip).start()
    for s in range(1, nt - 1):
        weight_partner(s)
    half_copy(chip).wait_recv()
    mine = part[piece(chip, core)] + halves[chip]
    for o in range(1, nchip):
        q = chip_peer(o)
        part_copy(q, q).wait_recv()
        mine += parts[q]
    right[piece(chip, core)] = mine * (1.0 / ndp)

    def right_copy(q_chip, q_core, target, send):
        place = right.at[piece(q_chip, q_core)]
        return copy(place, place, send, r_recv.at[2 * q_chip + q_core], dp=target)

    for o in range(1, nchip):
        q = chip_peer(o)
        right_copy(chip, core, 2 * q + core, r_send.at[q]).start()
    right_copy(chip, core, partner, t_send.at[chip]).start()
    weight_partner(nt - 1)

    b_high, b_low = split(basis)
    b_cat = jnp.concatenate([b_high, b_low, b_high], axis=1)

    def finish(cols):
        r = right[:, cols]
        high, low = split(r)
        approx = dot(b_cat, jnp.concatenate([high, high, low], axis=0))
        residual[:, cols] = (merged[:, cols] - approx).astype(BF16)
        factor[:, cols] = high

    if nrow == 1:
        finish(piece(chip, core)[1])

    for s in range(1, nt - 2):
        input_part(s)
    for o in range(1, nchip):
        q = chip_peer(o)
        right_copy(q, core, partner, r_send.at[q]).wait_recv()
        right_copy(q, core, partner, t_send.at[q]).start()
        if nrow == 1:
            finish(piece(q, core)[1])
    if nt > 2:
        input_part(nt - 2)
    for o in range(nchip):
        q = chip_peer(o)
        right_copy(q, 1 - core, partner, r_send.at[q]).wait_recv()
        if nrow == 1:
            finish(piece(q, 1 - core)[1])
    if nrow > 1:
        for c in range(ncol):
            finish(pl.ds(c * pw, pw))

    input_part(nt - 1)
    input_grad[...] = grad_sum[...].astype(BF16)

    for way in range(2):
        @pl.when(has_next(way))
        def _():
            for c in range(CHUNKS):
                token_copy(me, c, way).wait_send()
            weight_copy(me, way).wait_send()
        for s in range(1, nt):
            _, valid, b = origin(way, s)

            @pl.when(jnp.logical_and(valid, has_next(way)))
            def _():
                for c in range(CHUNKS):
                    token_copy(b, c, way).wait_send()
                weight_copy(b, way).wait_send()
    for z in range(1, nt):
        b = z_peer(z)
        copy(oall.at[b], oall.at[b], o_send.at[b], o_recv.at[b], tensor=b).wait_send()
        for o in range(chips):
            s = chip_slice(o)
            if o:
                chip_copy(b, o).wait_send()
            partner_copy(b, o).wait_send()
    for o in range(1, ndp):
        q = dp_peer(o)
        copy(lefts.at[dp], lefts.at[dp], l_send.at[q], l_recv.at[dp], dp=q).wait_send()
    for o in range(nchip):
        q = chip_peer(o)
        half_copy(q).wait_send()
        right_copy(q, core, partner, t_send.at[q]).wait_send()
        if o:
            part_copy(q, chip).wait_send()
            right_copy(chip, core, 2 * q + core, r_send.at[q]).wait_send()


def write_out(*refs):
    sems = refs[8]
    copies = []
    for i in range(4):
        src, dst = refs[i], refs[4 + i]
        count = PIECES if i == 0 else 2
        step = src.shape[0] // count
        for j in range(count):
            rows = pl.ds(j * step, step)
            copies.append(pltpu.make_async_copy(src.at[rows], dst.at[rows], sems.at[i, j]))
    for c in copies:
        c.start()
    for c in copies:
        c.wait()


def local(activations, out_grad, value_weight, error_feedback, warm_right):
    ndp, nt = lax.axis_size("dp"), lax.axis_size("tensor")
    layers = [[], [], [], []]
    for layer in range(activations.shape[0]):
        outs = one_layer(
            ndp, nt, activations[layer], out_grad[layer], value_weight[layer],
            error_feedback[layer, 0], warm_right[layer, 0].T,
        )
        for kept, out in zip(layers, outs):
            kept.append(out)
    residual, basis, factor, input_grad = [jnp.stack(kept) for kept in layers]
    return residual[:, None], basis.swapaxes(1, 2), factor.swapaxes(1, 2)[:, None], input_grad


def one_layer(ndp, nt, act, og, weight, error, warm):
    rows, width = act.shape
    tok, head = og.shape
    rank = warm.shape[0]
    spread = min(ndp, 8)
    ncol = min(ndp, width // 128)
    nrow = ndp // ncol
    dma = pltpu.SemaphoreType.DMA
    vmem = pl.BlockSpec(memory_space=pltpu.VMEM)
    shapes = (((head, width), BF16), ((rank, head), F32), ((rank, width), BF16), ((rows, width), BF16))
    results = pl.pallas_call(
        functools.partial(kernel, ndp, nt),
        out_shape=tuple(pltpu.VMEM(shape, dtype) for shape, dtype in shapes),
        in_specs=[pl.BlockSpec(memory_space=pltpu.HBM)] * 5,
        out_specs=(vmem,) * 4,
        scratch_shapes=[
            pltpu.VMEM((tok, head), BF16),
            pltpu.VMEM((head, width), BF16),
            pltpu.VMEM((rank, width), BF16),
            dma((5,)),
            pltpu.VMEM((rows, width), F32),
            pltpu.VMEM((tok, width), BF16),
            pltpu.VMEM((nt, head, width), BF16),
            pltpu.VMEM((nt, rows, head), BF16),
            pltpu.VMEM((head, width), F32),
            pltpu.VMEM((ndp, rank, head), F32),
            pltpu.VMEM((rank, width), F32),
            pltpu.VMEM((ndp // 2, rank // nrow, width // ncol), F32),
            pltpu.VMEM((ndp // 2, rank // nrow, width // ncol), F32),
            pltpu.VMEM((rank, width), F32),
            dma((2, nt, CHUNKS)), dma((nt, CHUNKS)),
            dma((2, nt)), dma((nt,)),
            dma((nt, spread)), dma((nt, spread)),
            dma((nt, spread)), dma((nt, spread)),
            dma((nt,)), dma((nt,)),
            dma((ndp,)), dma((ndp,)),
            dma((ndp // 2,)), dma((ndp // 2,)),
            dma((ndp // 2,)), dma((ndp // 2,)),
            dma((ndp // 2,)), dma((ndp,)), dma((ndp // 2,)),
        ],
        compiler_params=pltpu.CompilerParams(
            collective_id=0, has_side_effects=True, vmem_limit_bytes=62 * 1024 * 1024
        ),
    )(act, og, weight, error, warm)
    return pl.pallas_call(
        write_out,
        out_shape=tuple(jax.ShapeDtypeStruct(shape, dtype) for shape, dtype in shapes),
        in_specs=[vmem] * 4,
        out_specs=(pl.BlockSpec(memory_space=pltpu.HBM),) * 4,
        scratch_shapes=[dma((4, PIECES))],
        compiler_params=pltpu.CompilerParams(vmem_limit_bytes=16 * 1024 * 1024),
    )(*results)


def solution(mesh):
    return jax.shard_map(
        local,
        mesh=mesh,
        in_specs=(
            P(None, ("dp", "tensor"), None),
            P(None, "dp", "tensor"),
            P(None, "tensor", None),
            P(None, "dp", "tensor", None),
            P(None, "tensor", None, None),
        ),
        out_specs=(
            P(None, "dp", "tensor", None),
            P(None, "tensor", None),
            P(None, "tensor", None, None),
            P(None, ("dp", "tensor"), None),
        ),
        check_vma=False,
    )
```

```python
import functools

import jax
import jax.numpy as jnp
from jax import lax
from jax.experimental import pallas as pl
from jax.experimental.pallas import tpu as pltpu
from jax.sharding import PartitionSpec as P

MESH = pl.DeviceIdType.MESH
F32 = jnp.float32
BF16 = jnp.bfloat16
CHUNKS = 4
PIECES = 4
SUBS = 2


def split3(x):
    high = x.astype(BF16)
    rest = x - high.astype(F32)
    mid = rest.astype(BF16)
    return high, mid, (rest - mid.astype(F32)).astype(BF16)


def dot(a, b):
    return jnp.dot(a, b, preferred_element_type=F32)


def dot_nt(a, b):
    return lax.dot_general(a, b, (((1,), (1,)), ((), ())), preferred_element_type=F32)


def fold3(x):
    n = x.shape[0] // 3
    return x[:n] + x[n : 2 * n] + x[2 * n :]


def orthonormal(left):
    rank = left.shape[0]
    gram = lax.dot_general(
        left, left, (((1,), (1,)), ((), ())), precision=lax.Precision.HIGHEST, preferred_element_type=F32
    )
    row = lax.broadcasted_iota(jnp.int32, (rank, 1), 0)
    square = lax.broadcasted_iota(jnp.int32, (rank, rank), 0) == lax.broadcasted_iota(jnp.int32, (rank, rank), 1)
    gram = jnp.concatenate([gram, square.astype(F32)], axis=1)
    for k in range(rank):
        scale = lax.rsqrt(gram[k : k + 1, k : k + 1])
        gram_row = gram[k : k + 1, :] * scale
        left_row = left[k : k + 1, :] * scale
        column = jnp.where(row > k, gram[:, k : k + 1] * scale, 0.0)
        gram = jnp.where(row == k, gram_row, gram - column * gram_row)
        left = jnp.where(row == k, left_row, left - column * left_row)
    return left, gram[:, rank:]


def kernel(
    ndp, nt, act_hbm, og_hbm, weight_hbm, error_hbm, warm_hbm,
    residual, basis_out, factor, input_grad,
    og, stack, warm, wall, ogp, igs, merged, lefts, part, halves, parts, right,
    loads, act_send, act_recv, o_send, o_recv, g_send, g_recv, w_send, w_recv, i_send, i_recv,
    l_send, l_recv, h_send, h_recv, p_send, p_recv, r_send, r_recv, t_send, t_recv,
):
    dp = lax.axis_index("dp")
    me = lax.axis_index("tensor")
    rows, width = act_hbm.shape
    tok, head = og.shape
    rank = warm.shape[0]
    spread = ogp.shape[0]
    cw = width // CHUNKS
    wc = width // spread
    slot = lax.rem(dp, spread)
    group = dp - slot

    def copy(src, dst, send, recv, **device):
        return pltpu.make_async_remote_copy(
            src_ref=src, dst_ref=dst, send_sem=send, recv_sem=recv, device_id=device, device_id_type=MESH
        )

    def z_peer(o):
        return lax.rem(me + o, nt)

    def dp_peer(o):
        return lax.rem(dp + o, ndp)

    def group_peer(o):
        return lax.rem(slot + o, spread)

    def token_rows(b):
        return pl.ds(pl.multiple_of(b * rows, rows), rows)

    def slot_cols(s):
        return pl.ds(pl.multiple_of(s * wc, wc), wc)

    loading = [
        pltpu.make_async_copy(src, dst, loads.at[i])
        for i, (src, dst) in enumerate((
            (og_hbm, og), (act_hbm, stack.at[token_rows(me), :]), (og_hbm.at[token_rows(me), :], ogp.at[slot, me]),
            (warm_hbm, warm), (error_hbm, stack.at[pl.ds(tok, head), :]), (weight_hbm.at[:, slot_cols(slot)], wall.at[me]),
        ))
    ]
    for load in loading:
        load.start()

    barrier = pltpu.get_barrier_semaphore()
    for o in range(1, nt):
        pl.semaphore_signal(barrier, inc=1, device_id={"tensor": z_peer(o)}, device_id_type=MESH)
    for o in range(1, ndp):
        pl.semaphore_signal(barrier, inc=1, device_id={"dp": dp_peer(o)}, device_id_type=MESH)
    pl.semaphore_wait(barrier, nt + ndp - 2)

    def token_copy(b, c, way, s):
        place = stack.at[token_rows(b), pl.ds(c * cw, cw)]
        return copy(
            place, place, act_send.at[way, s], act_recv.at[b, c], tensor=jnp.clip(me + (1 - 2 * way), 0, nt - 1)
        )

    def has_next(way):
        return me < nt - 1 if way == 0 else me > 0

    def origin(way, s):
        b = me - s if way == 0 else me + s
        return b, (b >= 0 if way == 0 else b < nt), jnp.clip(b, 0, nt - 1)

    def weight_copy(q):
        return copy(wall.at[me], wall.at[me], w_send, w_recv.at[me], tensor=q)

    def send_weights(near, where):
        for way in range(2):
            for far in range(nt - 1, 0, -1):
                q = me + far if way == 0 else me - far
                valid = q < nt if way == 0 else q >= 0

                if (far == 1) == near:
                    @pl.when(jnp.logical_and(valid, where))
                    def _():
                        weight_copy(jnp.clip(q, 0, nt - 1)).start()

    at_end = jnp.logical_or(me == 0, me == nt - 1)
    inside = jnp.logical_not(at_end)

    loading[0].wait()
    for o in range(1, nt):
        q = z_peer(o)
        copy(og.at[token_rows(q), :], ogp.at[slot, me], o_send, o_recv, tensor=q).start()
    loading[1].wait()
    for c in range(CHUNKS):
        for way in range(2):
            @pl.when(has_next(way))
            def _():
                token_copy(me, c, way, 0).start()
    for load in loading[2:]:
        load.wait()
    send_weights(True, at_end)

    og_t = og[...].astype(F32).T.astype(BF16)
    left = dot_nt(warm[...], stack[tok:, :])

    inner = jnp.zeros((rank, tok), F32)
    for s in range(1, nt):
        for c in range(CHUNKS):
            for way in range(2):
                _, valid, b = origin(way, s)

                @pl.when(valid)
                def _():
                    token_copy(b, c, way, s).wait_recv()

                @pl.when(jnp.logical_and(valid, has_next(way)))
                def _():
                    token_copy(b, c, way, s).start()
            if s == 1 and c == 0:
                some = pl.ds(0, (nt - 1) * rows)
                copy(og.at[some, :], og.at[some, :], o_send, o_recv, tensor=z_peer(1)).wait_recv()
                for o in range(1, spread):
                    copy(ogp.at[slot], ogp.at[slot], g_send, g_recv, dp=group + group_peer(o)).start()
            if s == nt - 1:
                cols = slice(c * cw, (c + 1) * cw)
                inner += dot_nt(warm[:, cols], stack[:tok, cols])
                if c == CHUNKS // 2:
                    send_weights(False, at_end)

    left += fold3(dot(jnp.concatenate(split3(inner), axis=0), og[...]))
    lefts[dp] = left
    for o in range(1, ndp):
        copy(lefts.at[dp], lefts.at[dp], l_send, l_recv, dp=dp_peer(o)).start()
    send_weights(True, inside)

    for c in range(CHUNKS):
        cols = slice(c * cw, (c + 1) * cw)
        merged[:, cols] = dot(og_t, stack[:tok, cols]) + stack[tok:, cols].astype(F32)

    others = pl.ds(0, ndp - 1)
    copy(lefts.at[others], lefts.at[others], l_send, l_recv, dp=dp_peer(1)).wait_recv()
    send_weights(False, inside)
    total = lefts[0]
    for q in range(1, ndp):
        total += lefts[q]
    left = total * (1.0 / ndp)
    left_split = jnp.concatenate(split3(left), axis=0)
    inner_split = jnp.concatenate(split3(fold3(dot_nt(left_split, og[...]))), axis=0)
    lhs = jnp.concatenate([inner_split, left_split], axis=1)

    core = lax.rem(dp, 2)
    chip = dp // 2
    partner = dp + 1 - 2 * core
    nchip = ndp // 2
    ncol = min(ndp, width // 128)
    nrow = ndp // ncol
    pw, ph = width // ncol, rank // nrow
    subs, sub_rows = parts.shape[0], parts.shape[2]

    def piece(q_chip, q_core, sub=None):
        p = q_core * nchip + q_chip
        r, c = p // ncol, lax.rem(p, ncol)
        start, size = (0, ph) if sub is None else (sub * sub_rows, sub_rows)
        row = pl.ds(pl.multiple_of(r * ph + start, sub_rows), size) if nrow > 1 else pl.ds(start, size)
        return row, pl.ds(pl.multiple_of(c * pw, pw), pw)

    def chip_peer(o):
        return lax.rem(chip + o, nchip)

    def half_copy(i):
        return copy(part.at[piece(i, 1 - core)], halves.at[i], h_send, h_recv.at[i], dp=partner)

    def part_copy(q, sub):
        return copy(part.at[piece(q, core, sub)], parts.at[sub, chip], p_send, p_recv.at[sub], dp=2 * q + core)

    def compute_part(c):
        cols = pl.ds(pl.multiple_of(c * pw, pw), pw)
        part[:, cols] = fold3(dot(lhs, stack[:, cols]))

    if nrow == 1:
        for o in range(nchip):
            i = chip_peer(o + 1)
            compute_part((1 - core) * nchip + i)
            half_copy(i).start()
        for o in range(nchip):
            compute_part(core * nchip + chip_peer(o + 1))
    else:
        for c in range(ncol):
            compute_part(c)
        for o in range(nchip):
            half_copy(chip_peer(o + 1)).start()
    for o in range(1, nchip):
        q = chip_peer(o)
        half_copy(q).wait_recv()
        part[piece(q, core)] += halves[q]
        part_copy(q, 0).start()
    for sub in range(1, subs):
        for o in range(1, nchip):
            part_copy(chip_peer(o), sub).start()

    basis_t, inverse = orthonormal(left)
    basis_out[...] = basis_t
    outer = lax.dot_general(
        basis_t, inverse, (((0,), (0,)), ((), ())), precision=lax.Precision.HIGHEST, preferred_element_type=F32
    )
    high, mid, low = split3(jnp.concatenate([inverse, outer], axis=0))
    final = jnp.concatenate([high, high, mid, high, low, mid], axis=1)

    others = pl.ds(0, spread - 1)
    copy(ogp.at[others], ogp.at[others], g_send, g_recv, dp=partner).wait_recv()
    for o in range(1, nt):
        q = z_peer(o)
        copy(wall.at[q], wall.at[q], w_send, w_recv.at[q], tensor=q).wait_recv()
    grads = jnp.concatenate([ogp[:, b].reshape(spread * rows, head) for b in range(nt)], axis=1)
    igs[...] = dot(grads, wall[...].reshape(nt * head, wc)).astype(BF16).reshape(spread, rows, wc)

    def input_copy(q):
        return copy(igs.at[q], input_grad.at[:, slot_cols(slot)], i_send, i_recv, dp=group + q)

    half_copy(chip).wait_recv()

    def right_copy(q_chip, q_core, sub, target, send, recv):
        place = right.at[piece(q_chip, q_core, sub)]
        return copy(place, place, send, recv.at[sub, q_chip], dp=target)

    for sub in range(subs):
        some = pl.ds(0, nchip - 1)
        copy(parts.at[sub, some], parts.at[sub, some], p_send, p_recv.at[sub], dp=partner).wait_recv()
        mine = part[piece(chip, core, sub)] + halves[chip, sub * sub_rows : (sub + 1) * sub_rows]
        for o in range(1, nchip):
            mine += parts[sub, chip_peer(o)]
        right[piece(chip, core, sub)] = mine * (1.0 / ndp)
        for o in range(1, nchip):
            right_copy(chip, core, sub, 2 * chip_peer(o) + core, r_send, r_recv).start()
        right_copy(chip, core, sub, partner, t_send, t_recv).start()
    for o in range(1, spread):
        input_copy(group_peer(o)).start()
    input_grad[:, slot_cols(slot)] = igs[slot]

    def finish(cols):
        high, mid, low = split3(right[:, cols])
        out = dot(final, jnp.concatenate([high, mid, high, low, high, mid], axis=0))
        factor[:, cols] = out[:rank].astype(BF16)
        residual[:, cols] = (merged[:, cols] - out[rank:]).astype(BF16)

    if nrow == 1:
        finish(piece(chip, core)[1])
        for sub in range(subs):
            right_copy(chip, 1 - core, sub, partner, t_send, t_recv).wait_recv()
        finish(piece(chip, 1 - core)[1])
    for sub in range(subs):
        for o in range(1, nchip):
            q = chip_peer(o)
            right_copy(q, core, sub, partner, r_send, r_recv).wait_recv()
            right_copy(q, core, sub, partner, t_send, t_recv).start()
            if nrow == 1 and sub == subs - 1:
                finish(piece(q, core)[1])
    for o in range(1 if nrow == 1 else 0, nchip):
        q = chip_peer(o)
        for sub in range(subs):
            right_copy(q, 1 - core, sub, partner, t_send, t_recv).wait_recv()
        if nrow == 1:
            finish(piece(q, 1 - core)[1])
    if nrow > 1:
        for c in range(ncol):
            finish(pl.ds(c * pw, pw))

    others = pl.ds(0, spread - 1)
    copy(igs.at[others], igs.at[others], i_send, i_recv, dp=partner).wait_recv()

    for way in range(2):
        for s in range(nt):
            _, valid, b = origin(way, s)

            @pl.when(jnp.logical_and(valid, has_next(way)))
            def _():
                place = stack.at[token_rows(b), :]
                copy(place, place, act_send.at[way, s], act_recv.at[b, 0], tensor=z_peer(1)).wait_send()

    def sent(ref, send, recv):
        copy(ref, ref, send, recv, dp=partner).wait_send()

    sent(og.at[pl.ds(0, (nt - 1) * rows), :], o_send, o_recv)
    sent(ogp.at[others], g_send, g_recv)
    sent(wall.at[pl.ds(0, nt - 1)], w_send, w_recv.at[0])
    sent(igs.at[others], i_send, i_recv)
    sent(lefts.at[pl.ds(0, ndp - 1)], l_send, l_recv)
    sent(halves, h_send, h_recv.at[0])
    some = parts.at[:, pl.ds(0, nchip - 1)]
    sent(some, p_send, p_recv.at[0])
    sent(some, r_send, r_recv.at[0, 0])
    sent(halves, t_send, t_recv.at[0, 0])


def write_out(*refs):
    sems = refs[8]
    copies = []
    for i in range(4):
        src, dst = refs[i], refs[4 + i]
        count = PIECES if i == 0 else 2
        step = src.shape[0] // count
        for j in range(count):
            rows = pl.ds(j * step, step)
            copies.append(pltpu.make_async_copy(src.at[rows], dst.at[rows], sems.at[i, j]))
    for c in copies:
        c.start()
    for c in copies:
        c.wait()


def local(activations, out_grad, value_weight, error_feedback, warm_right):
    ndp, nt = lax.axis_size("dp"), lax.axis_size("tensor")
    layers = [[], [], [], []]
    for layer in range(activations.shape[0]):
        outs = one_layer(
            ndp, nt, activations[layer], out_grad[layer], value_weight[layer],
            error_feedback[layer, 0], warm_right[layer, 0].T,
        )
        for kept, out in zip(layers, outs):
            kept.append(out)
    residual, basis, factor, input_grad = [jnp.stack(kept) for kept in layers]
    return residual[:, None], basis.swapaxes(1, 2), factor.swapaxes(1, 2)[:, None], input_grad


def one_layer(ndp, nt, act, og, weight, error, warm):
    rows, width = act.shape
    tok, head = og.shape
    rank = warm.shape[0]
    spread = min(ndp, 8)
    ncol = min(ndp, width // 128)
    nrow = ndp // ncol
    nchip = ndp // 2
    ph, pw = rank // nrow, width // ncol
    subs = min(SUBS, ph // 8)
    dma = pltpu.SemaphoreType.DMA
    vmem = pl.BlockSpec(memory_space=pltpu.VMEM)
    shapes = (((head, width), BF16), ((rank, head), F32), ((rank, width), BF16), ((rows, width), BF16))
    results = pl.pallas_call(
        functools.partial(kernel, ndp, nt),
        out_shape=tuple(pltpu.VMEM(shape, dtype) for shape, dtype in shapes),
        in_specs=[pl.BlockSpec(memory_space=pltpu.HBM)] * 5,
        out_specs=(vmem,) * 4,
        scratch_shapes=[
            pltpu.VMEM((tok, head), BF16),
            pltpu.VMEM((tok + head, width), BF16),
            pltpu.VMEM((rank, width), BF16),
            pltpu.VMEM((nt, head, width // spread), BF16),
            pltpu.VMEM((spread, nt, rows, head), BF16),
            pltpu.VMEM((spread, rows, width // spread), BF16),
            pltpu.VMEM((head, width), F32),
            pltpu.VMEM((ndp, rank, head), F32),
            pltpu.VMEM((rank, width), F32),
            pltpu.VMEM((nchip, ph, pw), F32),
            pltpu.VMEM((subs, nchip, ph // subs, pw), F32),
            pltpu.VMEM((rank, width), F32),
            dma((6,)),
            dma((2, nt)), dma((nt, CHUNKS)),
            dma, dma, dma, dma,
            dma, dma((nt,)),
            dma, dma,
            dma, dma,
            dma, dma((nchip,)),
            dma, dma((subs,)),
            dma, dma((subs, nchip)),
            dma, dma((subs, nchip)),
        ],
        compiler_params=pltpu.CompilerParams(
            collective_id=0, has_side_effects=True, vmem_limit_bytes=62 * 1024 * 1024
        ),
    )(act, og, weight, error, warm)
    return pl.pallas_call(
        write_out,
        out_shape=tuple(jax.ShapeDtypeStruct(shape, dtype) for shape, dtype in shapes),
        in_specs=[vmem] * 4,
        out_specs=(pl.BlockSpec(memory_space=pltpu.HBM),) * 4,
        scratch_shapes=[dma((4, PIECES))],
        compiler_params=pltpu.CompilerParams(vmem_limit_bytes=16 * 1024 * 1024),
    )(*results)


def solution(mesh):
    return jax.shard_map(
        local,
        mesh=mesh,
        in_specs=(
            P(None, ("dp", "tensor"), None),
            P(None, "dp", "tensor"),
            P(None, "tensor", None),
            P(None, "dp", "tensor", None),
            P(None, "tensor", None, None),
        ),
        out_specs=(
            P(None, "dp", "tensor", None),
            P(None, "tensor", None),
            P(None, "tensor", None, None),
            P(None, ("dp", "tensor"), None),
        ),
        check_vma=False,
    )
```

```python
import functools

import jax
import jax.numpy as jnp
from jax import lax
from jax.experimental import pallas as pl
from jax.experimental.pallas import tpu as pltpu
from jax.sharding import PartitionSpec as P

MESH = pl.DeviceIdType.MESH
F32 = jnp.float32
BF16 = jnp.bfloat16
CHUNKS = 4
PIECES = 4
SUBS = 2
HELD = 2


def split3(x):
    high = x.astype(BF16)
    rest = x - high.astype(F32)
    mid = rest.astype(BF16)
    return high, mid, (rest - mid.astype(F32)).astype(BF16)


def dot(a, b):
    return jnp.dot(a, b, preferred_element_type=F32)


def dot_nt(a, b):
    return lax.dot_general(a, b, (((1,), (1,)), ((), ())), preferred_element_type=F32)


def fold3(x):
    n = x.shape[0] // 3
    return x[:n] + x[n : 2 * n] + x[2 * n :]


def orthonormal(left):
    rank = left.shape[0]
    gram = lax.dot_general(
        left, left, (((1,), (1,)), ((), ())), precision=lax.Precision.HIGHEST, preferred_element_type=F32
    )
    row = lax.broadcasted_iota(jnp.int32, (rank, 1), 0)
    square = lax.broadcasted_iota(jnp.int32, (rank, rank), 0) == lax.broadcasted_iota(jnp.int32, (rank, rank), 1)
    gram = jnp.concatenate([gram, square.astype(F32)], axis=1)
    for k in range(rank):
        scale = lax.rsqrt(gram[k : k + 1, k : k + 1])
        gram_row = gram[k : k + 1, :] * scale
        left_row = left[k : k + 1, :] * scale
        column = jnp.where(row > k, gram[:, k : k + 1] * scale, 0.0)
        gram = jnp.where(row == k, gram_row, gram - column * gram_row)
        left = jnp.where(row == k, left_row, left - column * left_row)
    return left, gram[:, rank:]


def kernel(
    ndp, nt, act_hbm, og_hbm, weight_hbm, error_hbm, warm_hbm,
    residual, basis_out, factor, input_grad,
    og, stack, warm, inner, told, wall, ogp, igs, merged, lefts, part, halves, parts, right,
    loads, act_send, act_recv, f_send, f_recv, n_send, n_recv, o_send, o_recv, g_send, g_recv, w_send, w_recv, i_send, i_recv,
    l_send, l_recv, h_send, h_recv, p_send, p_recv, r_send, r_recv, t_send, t_recv,
):
    dp = lax.axis_index("dp")
    me = lax.axis_index("tensor")
    rows, width = act_hbm.shape
    tok, head = og.shape
    rank = told.shape[0]
    spread = ogp.shape[0]
    cw = width // CHUNKS
    wc = width // spread
    slot = lax.rem(dp, spread)
    group = dp - slot

    def copy(src, dst, send, recv, **device):
        return pltpu.make_async_remote_copy(
            src_ref=src, dst_ref=dst, send_sem=send, recv_sem=recv, device_id=device, device_id_type=MESH
        )

    def z_peer(o):
        return lax.rem(me + o, nt)

    def dp_peer(o):
        return lax.rem(dp + o, ndp)

    def group_peer(o):
        return lax.rem(slot + o, spread)

    def token_rows(b):
        return pl.ds(pl.multiple_of(b * rows, rows), rows)

    def slot_cols(s):
        return pl.ds(pl.multiple_of(s * wc, wc), wc)

    loading = [
        pltpu.make_async_copy(src, dst, loads.at[i])
        for i, (src, dst) in enumerate((
            (og_hbm, og), (act_hbm, stack.at[token_rows(me), :]), (og_hbm.at[token_rows(me), :], ogp.at[slot, me]),
            (warm_hbm, warm.at[pl.ds(0, rank), :]), (error_hbm, stack.at[pl.ds(tok, head), :]), (weight_hbm.at[:, slot_cols(slot)], wall.at[me]),
        ))
    ]
    for load in loading:
        load.start()

    barrier = pltpu.get_barrier_semaphore()
    for o in range(1, nt):
        pl.semaphore_signal(barrier, inc=1, device_id={"tensor": z_peer(o)}, device_id_type=MESH)
    for o in range(1, ndp):
        pl.semaphore_signal(barrier, inc=1, device_id={"dp": dp_peer(o)}, device_id_type=MESH)
    pl.semaphore_wait(barrier, nt + ndp - 2)

    def token_copy(b, c, way, s):
        place = stack.at[token_rows(b), pl.ds(c * cw, cw)]
        return copy(
            place, place, act_send.at[way, s], act_recv.at[b, c], tensor=jnp.clip(me + (1 - 2 * way), 0, nt - 1)
        )

    def has_next(way):
        return me < nt - 1 if way == 0 else me > 0

    def origin(way, s):
        b = me - s if way == 0 else me + s
        return b, (b >= 0 if way == 0 else b < nt), jnp.clip(b, 0, nt - 1)

    def weight_copy(q):
        return copy(wall.at[me], wall.at[me], w_send, w_recv.at[me], tensor=q)

    def send_weights(near, where):
        for way in range(2):
            for far in range(nt - 1, 0, -1):
                q = me + far if way == 0 else me - far
                valid = q < nt if way == 0 else q >= 0

                if (far == 1) == near:
                    @pl.when(valid if where is True else jnp.logical_and(valid, where))
                    def _():
                        weight_copy(jnp.clip(q, 0, nt - 1)).start()

    at_end = jnp.logical_or(me == 0, me == nt - 1)
    inside = jnp.logical_not(at_end)
    core = lax.rem(dp, 2)
    partner = dp + 1 - 2 * core
    helped = nt == 4
    neighbour = jnp.where(me == 0, 1, jnp.where(me == nt - 1, nt - 2, jnp.where(me == 1, 0, nt - 1)))

    def warm_half(which):
        return pl.ds(pl.multiple_of(which * (width // 2), width // 2), width // 2)

    def warm_copy(**device):
        src = warm.at[pl.ds(0, rank), warm_half(core)]
        return copy(src, warm.at[pl.ds(rank, rank), warm_half(core)], f_send, f_recv.at[0], **device)

    def warm_share(which):
        place = warm.at[pl.ds(rank, rank), warm_half(which)]
        return copy(place, place, f_send, f_recv.at[1], dp=partner)

    def told_copy():
        return copy(inner.at[pl.ds(rank, rank), :], told, n_send, n_recv, tensor=neighbour)

    loading[0].wait()
    for o in range(1, nt):
        q = z_peer(o)
        copy(og.at[token_rows(q), :], ogp.at[slot, me], o_send, o_recv, tensor=q).start()
    loading[1].wait()
    for c in range(CHUNKS):
        for way in range(2):
            @pl.when(has_next(way))
            def _():
                token_copy(me, c, way, 0).start()
    for load in loading[2:]:
        load.wait()
    if helped:
        @pl.when(at_end)
        def _():
            warm_copy(tensor=neighbour).start()
    send_weights(True, at_end)

    og_t = og[...].astype(F32).T.astype(BF16)
    left_error = dot_nt(warm[:rank, :], stack[tok:, :])

    def send_left(product):
        lefts[dp] = left_error + fold3(dot(jnp.concatenate(split3(product), axis=0), og[...]))
        for o in range(1, ndp):
            copy(lefts.at[dp], lefts.at[dp], l_send, l_recv, dp=dp_peer(o)).start()

    for s in range(1, nt):
        help_now = helped and s == nt - 2
        for c in range(CHUNKS):
            for way in range(2):
                _, valid, b = origin(way, s)

                @pl.when(valid)
                def _():
                    token_copy(b, c, way, s).wait_recv()

                if not (help_now and c >= HELD):
                    @pl.when(jnp.logical_and(valid, has_next(way)))
                    def _():
                        token_copy(b, c, way, s).start()
            if s == 1 and c == 0:
                some = pl.ds(0, (nt - 1) * rows)
                copy(og.at[some, :], og.at[some, :], o_send, o_recv, tensor=z_peer(1)).wait_recv()
                for o in range(1, spread):
                    copy(ogp.at[slot], ogp.at[slot], g_send, g_recv, dp=group + group_peer(o)).start()
            if help_now and c == HELD - 1:
                @pl.when(inside)
                def _():
                    warm_copy(tensor=neighbour).wait_recv()
                    warm_share(core).start()
            if help_now and c == CHUNKS - 2:
                @pl.when(inside)
                def _():
                    warm_share(1 - core).wait_recv()
                    inner[...] = dot_nt(warm[:, : (c + 1) * cw], stack[:tok, : (c + 1) * cw])
            if s == nt - 1 and c == CHUNKS // 2 - 1 and helped:
                @pl.when(at_end)
                def _():
                    told_copy().wait_recv()
                    send_left(told[...])
            if s == nt - 1 and c == CHUNKS // 2:
                send_weights(False, at_end)
        if help_now:
            @pl.when(inside)
            def _():
                last = slice((CHUNKS - 1) * cw, width)
                inner[...] += dot_nt(warm[:, last], stack[:tok, last])
                told_copy().start()
            for c in range(HELD, CHUNKS):
                for way in range(2):
                    _, valid, b = origin(way, s)

                    @pl.when(jnp.logical_and(valid, has_next(way)))
                    def _():
                        token_copy(b, c, way, s).start()

            @pl.when(inside)
            def _():
                send_left(inner[:rank, :])
                send_weights(True, True)
    if not helped:
        send_left(dot_nt(warm[:rank, :], stack[:tok, :]))
        send_weights(True, inside)

    for c in range(CHUNKS):
        cols = slice(c * cw, (c + 1) * cw)
        merged[:, cols] = dot(og_t, stack[:tok, cols]) + stack[tok:, cols].astype(F32)

    others = pl.ds(0, ndp - 1)
    copy(lefts.at[others], lefts.at[others], l_send, l_recv, dp=dp_peer(1)).wait_recv()
    send_weights(False, inside)
    total = lefts[0]
    for q in range(1, ndp):
        total += lefts[q]
    left = total * (1.0 / ndp)
    left_split = jnp.concatenate(split3(left), axis=0)
    inner_split = jnp.concatenate(split3(fold3(dot_nt(left_split, og[...]))), axis=0)
    lhs = jnp.concatenate([inner_split, left_split], axis=1)

    chip = dp // 2
    nchip = ndp // 2
    ncol = min(ndp, width // 128)
    nrow = ndp // ncol
    pw, ph = width // ncol, rank // nrow
    subs, sub_rows = parts.shape[0], parts.shape[2]

    def piece(q_chip, q_core, sub=None):
        p = q_core * nchip + q_chip
        r, c = p // ncol, lax.rem(p, ncol)
        start, size = (0, ph) if sub is None else (sub * sub_rows, sub_rows)
        row = pl.ds(pl.multiple_of(r * ph + start, sub_rows), size) if nrow > 1 else pl.ds(start, size)
        return row, pl.ds(pl.multiple_of(c * pw, pw), pw)

    def chip_peer(o):
        return lax.rem(chip + o, nchip)

    def half_copy(i):
        return copy(part.at[piece(i, 1 - core)], halves.at[i], h_send, h_recv.at[i], dp=partner)

    def part_copy(q, sub):
        return copy(part.at[piece(q, core, sub)], parts.at[sub, chip], p_send, p_recv.at[sub], dp=2 * q + core)

    def compute_part(c):
        cols = pl.ds(pl.multiple_of(c * pw, pw), pw)
        part[:, cols] = fold3(dot(lhs, stack[:, cols]))

    if nrow == 1:
        for o in range(nchip):
            i = chip_peer(o + 1)
            compute_part((1 - core) * nchip + i)
            half_copy(i).start()
        for o in range(nchip):
            compute_part(core * nchip + chip_peer(o + 1))
    else:
        for c in range(ncol):
            compute_part(c)
        for o in range(nchip):
            half_copy(chip_peer(o + 1)).start()
    for o in range(1, nchip):
        q = chip_peer(o)
        half_copy(q).wait_recv()
        part[piece(q, core)] += halves[q]
        part_copy(q, 0).start()
    for sub in range(1, subs):
        for o in range(1, nchip):
            part_copy(chip_peer(o), sub).start()

    basis_t, inverse = orthonormal(left)
    basis_out[...] = basis_t
    outer = lax.dot_general(
        basis_t, inverse, (((0,), (0,)), ((), ())), precision=lax.Precision.HIGHEST, preferred_element_type=F32
    )
    high, mid, low = split3(jnp.concatenate([inverse, outer], axis=0))
    final = jnp.concatenate([high, high, mid, high, low, mid], axis=1)

    half_copy(chip).wait_recv()

    def right_copy(q_chip, q_core, sub, target, send, recv):
        place = right.at[piece(q_chip, q_core, sub)]
        return copy(place, place, send, recv.at[sub, q_chip], dp=target)

    for sub in range(subs):
        some = pl.ds(0, nchip - 1)
        copy(parts.at[sub, some], parts.at[sub, some], p_send, p_recv.at[sub], dp=partner).wait_recv()
        mine = part[piece(chip, core, sub)] + halves[chip, sub * sub_rows : (sub + 1) * sub_rows]
        for o in range(1, nchip):
            mine += parts[sub, chip_peer(o)]
        right[piece(chip, core, sub)] = mine * (1.0 / ndp)
        for o in range(1, nchip):
            right_copy(chip, core, sub, 2 * chip_peer(o) + core, r_send, r_recv).start()
        right_copy(chip, core, sub, partner, t_send, t_recv).start()
    others = pl.ds(0, spread - 1)
    copy(ogp.at[others], ogp.at[others], g_send, g_recv, dp=partner).wait_recv()
    for o in range(1, nt):
        q = z_peer(o)
        copy(wall.at[q], wall.at[q], w_send, w_recv.at[q], tensor=q).wait_recv()
    grads = jnp.concatenate([ogp[:, b].reshape(spread * rows, head) for b in range(nt)], axis=1)
    igs[...] = dot(grads, wall[...].reshape(nt * head, wc)).astype(BF16).reshape(spread, rows, wc)

    def input_copy(q):
        return copy(igs.at[q], input_grad.at[:, slot_cols(slot)], i_send, i_recv, dp=group + q)

    for o in range(1, spread):
        input_copy(group_peer(o)).start()
    input_grad[:, slot_cols(slot)] = igs[slot]

    def finish(cols):
        high, mid, low = split3(right[:, cols])
        out = dot(final, jnp.concatenate([high, mid, high, low, high, mid], axis=0))
        factor[:, cols] = out[:rank].astype(BF16)
        residual[:, cols] = (merged[:, cols] - out[rank:]).astype(BF16)

    if nrow == 1:
        finish(piece(chip, core)[1])
        for sub in range(subs):
            right_copy(chip, 1 - core, sub, partner, t_send, t_recv).wait_recv()
        finish(piece(chip, 1 - core)[1])
    for sub in range(subs):
        for o in range(1, nchip):
            q = chip_peer(o)
            right_copy(q, core, sub, partner, r_send, r_recv).wait_recv()
            right_copy(q, core, sub, partner, t_send, t_recv).start()
            if nrow == 1 and sub == subs - 1:
                finish(piece(q, core)[1])
    for o in range(1 if nrow == 1 else 0, nchip):
        q = chip_peer(o)
        for sub in range(subs):
            right_copy(q, 1 - core, sub, partner, t_send, t_recv).wait_recv()
        if nrow == 1:
            finish(piece(q, 1 - core)[1])
    if nrow > 1:
        for c in range(ncol):
            finish(pl.ds(c * pw, pw))

    others = pl.ds(0, spread - 1)
    copy(igs.at[others], igs.at[others], i_send, i_recv, dp=partner).wait_recv()

    for way in range(2):
        for s in range(nt):
            _, valid, b = origin(way, s)

            @pl.when(jnp.logical_and(valid, has_next(way)))
            def _():
                place = stack.at[token_rows(b), :]
                copy(place, place, act_send.at[way, s], act_recv.at[b, 0], tensor=z_peer(1)).wait_send()

    def sent(ref, send, recv):
        copy(ref, ref, send, recv, dp=partner).wait_send()

    if helped:
        @pl.when(at_end)
        def _():
            copy(warm.at[pl.ds(0, rank), warm_half(0)], warm.at[pl.ds(0, rank), warm_half(0)], f_send, f_recv.at[0], dp=partner).wait_send()

        @pl.when(inside)
        def _():
            warm_share(core).wait_send()
            told_copy().wait_send()

    sent(og.at[pl.ds(0, (nt - 1) * rows), :], o_send, o_recv)
    sent(ogp.at[others], g_send, g_recv)
    sent(wall.at[pl.ds(0, nt - 1)], w_send, w_recv.at[0])
    sent(igs.at[others], i_send, i_recv)
    sent(lefts.at[pl.ds(0, ndp - 1)], l_send, l_recv)
    sent(halves, h_send, h_recv.at[0])
    some = parts.at[:, pl.ds(0, nchip - 1)]
    sent(some, p_send, p_recv.at[0])
    sent(some, r_send, r_recv.at[0, 0])
    sent(halves, t_send, t_recv.at[0, 0])


def write_out(*refs):
    sems = refs[8]
    copies = []
    for i in range(4):
        src, dst = refs[i], refs[4 + i]
        count = PIECES if i == 0 else 2
        step = src.shape[0] // count
        for j in range(count):
            rows = pl.ds(j * step, step)
            copies.append(pltpu.make_async_copy(src.at[rows], dst.at[rows], sems.at[i, j]))
    for c in copies:
        c.start()
    for c in copies:
        c.wait()


def local(activations, out_grad, value_weight, error_feedback, warm_right):
    ndp, nt = lax.axis_size("dp"), lax.axis_size("tensor")
    layers = [[], [], [], []]
    for layer in range(activations.shape[0]):
        outs = one_layer(
            ndp, nt, activations[layer], out_grad[layer], value_weight[layer],
            error_feedback[layer, 0], warm_right[layer, 0].T,
        )
        for kept, out in zip(layers, outs):
            kept.append(out)
    residual, basis, factor, input_grad = [jnp.stack(kept) for kept in layers]
    return residual[:, None], basis.swapaxes(1, 2), factor.swapaxes(1, 2)[:, None], input_grad


def one_layer(ndp, nt, act, og, weight, error, warm):
    rows, width = act.shape
    tok, head = og.shape
    rank = warm.shape[0]
    spread = min(ndp, 8)
    ncol = min(ndp, width // 128)
    nrow = ndp // ncol
    nchip = ndp // 2
    ph, pw = rank // nrow, width // ncol
    subs = min(SUBS, ph // 8)
    dma = pltpu.SemaphoreType.DMA
    vmem = pl.BlockSpec(memory_space=pltpu.VMEM)
    shapes = (((head, width), BF16), ((rank, head), F32), ((rank, width), BF16), ((rows, width), BF16))
    results = pl.pallas_call(
        functools.partial(kernel, ndp, nt),
        out_shape=tuple(pltpu.VMEM(shape, dtype) for shape, dtype in shapes),
        in_specs=[pl.BlockSpec(memory_space=pltpu.HBM)] * 5,
        out_specs=(vmem,) * 4,
        scratch_shapes=[
            pltpu.VMEM((tok, head), BF16),
            pltpu.VMEM((tok + head, width), BF16),
            pltpu.VMEM((2 * rank, width), BF16),
            pltpu.VMEM((2 * rank, tok), F32),
            pltpu.VMEM((rank, tok), F32),
            pltpu.VMEM((nt, head, width // spread), BF16),
            pltpu.VMEM((spread, nt, rows, head), BF16),
            pltpu.VMEM((spread, rows, width // spread), BF16),
            pltpu.VMEM((head, width), F32),
            pltpu.VMEM((ndp, rank, head), F32),
            pltpu.VMEM((rank, width), F32),
            pltpu.VMEM((nchip, ph, pw), F32),
            pltpu.VMEM((subs, nchip, ph // subs, pw), F32),
            pltpu.VMEM((rank, width), F32),
            dma((6,)),
            dma((2, nt)), dma((nt, CHUNKS)),
            dma, dma((2,)), dma, dma,
            dma, dma, dma, dma,
            dma, dma((nt,)),
            dma, dma,
            dma, dma,
            dma, dma((nchip,)),
            dma, dma((subs,)),
            dma, dma((subs, nchip)),
            dma, dma((subs, nchip)),
        ],
        compiler_params=pltpu.CompilerParams(
            collective_id=0, has_side_effects=True, vmem_limit_bytes=62 * 1024 * 1024
        ),
    )(act, og, weight, error, warm)
    return pl.pallas_call(
        write_out,
        out_shape=tuple(jax.ShapeDtypeStruct(shape, dtype) for shape, dtype in shapes),
        in_specs=[vmem] * 4,
        out_specs=(pl.BlockSpec(memory_space=pltpu.HBM),) * 4,
        scratch_shapes=[dma((4, PIECES))],
        compiler_params=pltpu.CompilerParams(vmem_limit_bytes=16 * 1024 * 1024),
    )(*results)


def solution(mesh):
    return jax.shard_map(
        local,
        mesh=mesh,
        in_specs=(
            P(None, ("dp", "tensor"), None),
            P(None, "dp", "tensor"),
            P(None, "tensor", None),
            P(None, "dp", "tensor", None),
            P(None, "tensor", None, None),
        ),
        out_specs=(
            P(None, "dp", "tensor", None),
            P(None, "tensor", None),
            P(None, "tensor", None, None),
            P(None, ("dp", "tensor"), None),
        ),
        check_vma=False,
    )
```

```python
import functools

import jax
import jax.numpy as jnp
from jax import lax
from jax.experimental import pallas as pl
from jax.experimental.pallas import tpu as pltpu
from jax.sharding import PartitionSpec as P

MESH = pl.DeviceIdType.MESH
F32 = jnp.float32
BF16 = jnp.bfloat16
CHUNKS = 4
PIECES = 4
SUBS = 4
HELD = 2


def split3(x):
    high = x.astype(BF16)
    rest = x - high.astype(F32)
    mid = rest.astype(BF16)
    return high, mid, (rest - mid.astype(F32)).astype(BF16)


def dot(a, b):
    return jnp.dot(a, b, preferred_element_type=F32)


def dot_nt(a, b):
    return lax.dot_general(a, b, (((1,), (1,)), ((), ())), preferred_element_type=F32)


def fold3(x):
    n = x.shape[0] // 3
    return x[:n] + x[n : 2 * n] + x[2 * n :]


def orthonormal(left):
    rank = left.shape[0]
    gram = lax.dot_general(
        left, left, (((1,), (1,)), ((), ())), precision=lax.Precision.HIGHEST, preferred_element_type=F32
    )
    row = lax.broadcasted_iota(jnp.int32, (rank, 1), 0)
    square = lax.broadcasted_iota(jnp.int32, (rank, rank), 0) == lax.broadcasted_iota(jnp.int32, (rank, rank), 1)
    gram = jnp.concatenate([gram, square.astype(F32)], axis=1)
    for k in range(rank):
        scale = lax.rsqrt(gram[k : k + 1, k : k + 1])
        gram_row = gram[k : k + 1, :] * scale
        left_row = left[k : k + 1, :] * scale
        column = jnp.where(row > k, gram[:, k : k + 1] * scale, 0.0)
        gram = jnp.where(row == k, gram_row, gram - column * gram_row)
        left = jnp.where(row == k, left_row, left - column * left_row)
    return left, gram[:, rank:]


def kernel(
    ndp, nt, act_hbm, og_hbm, weight_hbm, error_hbm, warm_hbm,
    residual, basis_out, factor, input_grad,
    og, stack, warm, inner, told, wall, ogp, igs, merged, lefts, part, halves, parts, right,
    loads, act_send, act_recv, f_send, f_recv, n_send, n_recv, o_send, o_recv, g_send, g_recv, w_send, w_recv, i_send, i_recv,
    l_send, l_recv, h_send, h_recv, p_send, p_recv, r_send, r_recv, t_send, t_recv,
):
    dp = lax.axis_index("dp")
    me = lax.axis_index("tensor")
    rows, width = act_hbm.shape
    tok, head = og.shape
    rank = told.shape[0]
    spread = ogp.shape[0]
    cw = width // CHUNKS
    wc = width // spread
    slot = lax.rem(dp, spread)
    group = dp - slot

    def copy(src, dst, send, recv, **device):
        return pltpu.make_async_remote_copy(
            src_ref=src, dst_ref=dst, send_sem=send, recv_sem=recv, device_id=device, device_id_type=MESH
        )

    def issue(*copies):
        @pl.when(dp >= 0)
        def _():
            for c in copies:
                c.start()

    def z_peer(o):
        return lax.rem(me + o, nt)

    def dp_peer(o):
        return lax.rem(dp + o, ndp)

    def group_peer(o):
        return lax.rem(slot + o, spread)

    def token_rows(b):
        return pl.ds(pl.multiple_of(b * rows, rows), rows)

    def slot_cols(s):
        return pl.ds(pl.multiple_of(s * wc, wc), wc)

    loading = [
        pltpu.make_async_copy(src, dst, loads.at[i])
        for i, (src, dst) in enumerate((
            (og_hbm, og), (act_hbm, stack.at[token_rows(me), :]), (og_hbm.at[token_rows(me), :], ogp.at[slot, me]),
            (warm_hbm, warm.at[pl.ds(0, rank), :]), (error_hbm, stack.at[pl.ds(tok, head), :]), (weight_hbm.at[:, slot_cols(slot)], wall.at[me]),
        ))
    ]
    for load in loading:
        load.start()

    barrier = pltpu.get_barrier_semaphore()
    for o in range(1, nt):
        pl.semaphore_signal(barrier, inc=1, device_id={"tensor": z_peer(o)}, device_id_type=MESH)
    for o in range(1, ndp):
        pl.semaphore_signal(barrier, inc=1, device_id={"dp": dp_peer(o)}, device_id_type=MESH)
    pl.semaphore_wait(barrier, nt + ndp - 2)

    def token_copy(b, c, way, s):
        place = stack.at[token_rows(b), pl.ds(c * cw, cw)]
        return copy(
            place, place, act_send.at[way, s], act_recv.at[b, c], tensor=jnp.clip(me + (1 - 2 * way), 0, nt - 1)
        )

    def has_next(way):
        return me < nt - 1 if way == 0 else me > 0

    def origin(way, s):
        b = me - s if way == 0 else me + s
        return b, (b >= 0 if way == 0 else b < nt), jnp.clip(b, 0, nt - 1)

    def weight_copy(q):
        return copy(wall.at[me], wall.at[me], w_send, w_recv.at[me], tensor=q)

    def send_weights(near, where):
        for way in range(2):
            for far in range(nt - 1, 0, -1):
                q = me + far if way == 0 else me - far
                valid = q < nt if way == 0 else q >= 0

                if (far == 1) == near:
                    @pl.when(valid if where is True else jnp.logical_and(valid, where))
                    def _():
                        weight_copy(jnp.clip(q, 0, nt - 1)).start()

    at_end = jnp.logical_or(me == 0, me == nt - 1)
    inside = jnp.logical_not(at_end)
    core = lax.rem(dp, 2)
    partner = dp + 1 - 2 * core
    helped = nt == 4
    neighbour = jnp.where(me == 0, 1, jnp.where(me == nt - 1, nt - 2, jnp.where(me == 1, 0, nt - 1)))

    def warm_half(which):
        return pl.ds(pl.multiple_of(which * (width // 2), width // 2), width // 2)

    def warm_copy(**device):
        src = warm.at[pl.ds(0, rank), warm_half(core)]
        return copy(src, warm.at[pl.ds(rank, rank), warm_half(core)], f_send, f_recv.at[0], **device)

    def warm_share(which):
        place = warm.at[pl.ds(rank, rank), warm_half(which)]
        return copy(place, place, f_send, f_recv.at[1], dp=partner)

    def told_copy():
        return copy(inner.at[pl.ds(rank, rank), :], told, n_send, n_recv, tensor=neighbour)

    loading[0].wait()
    issue(*(
        copy(og.at[token_rows(z_peer(o)), :], ogp.at[slot, me], o_send, o_recv, tensor=z_peer(o)) for o in range(1, nt)
    ))
    loading[1].wait()
    for c in range(CHUNKS):
        for way in range(2):
            @pl.when(has_next(way))
            def _():
                token_copy(me, c, way, 0).start()
    for load in loading[2:]:
        load.wait()
    if helped:
        @pl.when(at_end)
        def _():
            warm_copy(tensor=neighbour).start()
    send_weights(True, at_end)

    og_t = og[...].astype(F32).T.astype(BF16)
    left_error = dot_nt(warm[:rank, :], stack[tok:, :])

    def send_left(product):
        lefts[dp] = left_error + fold3(dot(jnp.concatenate(split3(product), axis=0), og[...]))
        issue(*(copy(lefts.at[dp], lefts.at[dp], l_send, l_recv, dp=dp_peer(o)) for o in range(1, ndp)))

    for s in range(1, nt):
        help_now = helped and s == nt - 2
        for c in range(CHUNKS):
            for way in range(2):
                _, valid, b = origin(way, s)

                @pl.when(valid)
                def _():
                    token_copy(b, c, way, s).wait_recv()

                if not (help_now and c >= HELD):
                    @pl.when(jnp.logical_and(valid, has_next(way)))
                    def _():
                        token_copy(b, c, way, s).start()
            if s == 1 and c == 0:
                some = pl.ds(0, (nt - 1) * rows)
                copy(og.at[some, :], og.at[some, :], o_send, o_recv, tensor=z_peer(1)).wait_recv()
                issue(*(
                    copy(ogp.at[slot], ogp.at[slot], g_send, g_recv, dp=group + group_peer(o)) for o in range(1, spread)
                ))
            if help_now and c == HELD - 1:
                @pl.when(inside)
                def _():
                    warm_copy(tensor=neighbour).wait_recv()
                    warm_share(core).start()
            if help_now and c == CHUNKS - 2:
                @pl.when(inside)
                def _():
                    warm_share(1 - core).wait_recv()
                    inner[...] = dot_nt(warm[:, : (c + 1) * cw], stack[:tok, : (c + 1) * cw])
            if s == nt - 1 and c == CHUNKS // 2 - 1 and helped:
                @pl.when(at_end)
                def _():
                    told_copy().wait_recv()
                    send_left(told[...])
            if s == nt - 1 and c == CHUNKS // 2:
                send_weights(False, at_end)
        if help_now:
            @pl.when(inside)
            def _():
                last = slice((CHUNKS - 1) * cw, width)
                inner[...] += dot_nt(warm[:, last], stack[:tok, last])
                told_copy().start()
            for c in range(HELD, CHUNKS):
                for way in range(2):
                    _, valid, b = origin(way, s)

                    @pl.when(jnp.logical_and(valid, has_next(way)))
                    def _():
                        token_copy(b, c, way, s).start()

            @pl.when(inside)
            def _():
                send_left(inner[:rank, :])
                send_weights(True, True)
    if not helped:
        send_left(dot_nt(warm[:rank, :], stack[:tok, :]))
        send_weights(True, inside)

    for c in range(CHUNKS):
        cols = slice(c * cw, (c + 1) * cw)
        merged[:, cols] = dot(og_t, stack[:tok, cols]) + stack[tok:, cols].astype(F32)

    others = pl.ds(0, ndp - 1)
    copy(lefts.at[others], lefts.at[others], l_send, l_recv, dp=dp_peer(1)).wait_recv()
    send_weights(False, inside)
    total = lefts[0]
    for q in range(1, ndp):
        total += lefts[q]
    left = total * (1.0 / ndp)
    left_split = jnp.concatenate(split3(left), axis=0)
    inner_split = jnp.concatenate(split3(fold3(dot_nt(left_split, og[...]))), axis=0)
    lhs = jnp.concatenate([inner_split, left_split], axis=1)

    chip = dp // 2
    nchip = ndp // 2
    ncol = min(ndp, width // 128)
    nrow = ndp // ncol
    pw, ph = width // ncol, rank // nrow
    subs, sub_rows = parts.shape[0], parts.shape[2]

    def piece(q_chip, q_core, sub=None):
        p = q_core * nchip + q_chip
        r, c = p // ncol, lax.rem(p, ncol)
        start, size = (0, ph) if sub is None else (sub * sub_rows, sub_rows)
        row = pl.ds(pl.multiple_of(r * ph + start, sub_rows), size) if nrow > 1 else pl.ds(start, size)
        return row, pl.ds(pl.multiple_of(c * pw, pw), pw)

    def chip_peer(o):
        return lax.rem(chip + o, nchip)

    def half_copy(i):
        return copy(part.at[piece(i, 1 - core)], halves.at[i], h_send, h_recv.at[i], dp=partner)

    def part_copy(q, sub):
        return copy(part.at[piece(q, core, sub)], parts.at[sub, chip], p_send, p_recv.at[sub], dp=2 * q + core)

    def compute_part(c):
        cols = pl.ds(pl.multiple_of(c * pw, pw), pw)
        part[:, cols] = fold3(dot(lhs, stack[:, cols]))

    if nrow == 1:
        for o in range(nchip):
            i = chip_peer(o + 1)
            compute_part((1 - core) * nchip + i)
            issue(half_copy(i))
        for o in range(nchip):
            compute_part(core * nchip + chip_peer(o + 1))
    else:
        for c in range(ncol):
            compute_part(c)
        issue(*(half_copy(chip_peer(o + 1)) for o in range(nchip)))
    for o in range(1, nchip):
        q = chip_peer(o)
        half_copy(q).wait_recv()
        part[piece(q, core)] += halves[q]
        issue(part_copy(q, 0))
    issue(*(part_copy(chip_peer(o), sub) for sub in range(1, subs) for o in range(1, nchip)))

    basis_t, inverse = orthonormal(left)
    basis_out[...] = basis_t
    outer = lax.dot_general(
        basis_t, inverse, (((0,), (0,)), ((), ())), precision=lax.Precision.HIGHEST, preferred_element_type=F32
    )
    high, mid, low = split3(jnp.concatenate([inverse, outer], axis=0))
    final = jnp.concatenate([high, high, mid, high, low, mid], axis=1)

    half_copy(chip).wait_recv()

    def right_copy(q_chip, q_core, sub, target, send, recv):
        place = right.at[piece(q_chip, q_core, sub)]
        return copy(place, place, send, recv.at[sub, q_chip], dp=target)

    for sub in range(subs):
        some = pl.ds(0, nchip - 1)
        copy(parts.at[sub, some], parts.at[sub, some], p_send, p_recv.at[sub], dp=partner).wait_recv()
        mine = part[piece(chip, core, sub)] + halves[chip, sub * sub_rows : (sub + 1) * sub_rows]
        for o in range(1, nchip):
            mine += parts[sub, chip_peer(o)]
        right[piece(chip, core, sub)] = mine * (1.0 / ndp)
        issue(
            *(right_copy(chip, core, sub, 2 * chip_peer(o) + core, r_send, r_recv) for o in range(1, nchip)),
            right_copy(chip, core, sub, partner, t_send, t_recv),
        )
    others = pl.ds(0, spread - 1)
    copy(ogp.at[others], ogp.at[others], g_send, g_recv, dp=partner).wait_recv()
    for o in range(1, nt):
        q = z_peer(o)
        copy(wall.at[q], wall.at[q], w_send, w_recv.at[q], tensor=q).wait_recv()
    grads = jnp.concatenate([ogp[:, b].reshape(spread * rows, head) for b in range(nt)], axis=1)
    igs[...] = dot(grads, wall[...].reshape(nt * head, wc)).astype(BF16).reshape(spread, rows, wc)

    def input_copy(q):
        return copy(igs.at[q], input_grad.at[:, slot_cols(slot)], i_send, i_recv, dp=group + q)

    issue(*(input_copy(group_peer(o)) for o in range(1, spread)))
    input_grad[:, slot_cols(slot)] = igs[slot]

    def finish(cols):
        high, mid, low = split3(right[:, cols])
        out = dot(final, jnp.concatenate([high, mid, high, low, high, mid], axis=0))
        factor[:, cols] = out[:rank].astype(BF16)
        residual[:, cols] = (merged[:, cols] - out[rank:]).astype(BF16)

    if nrow == 1:
        finish(piece(chip, core)[1])
        for sub in range(subs):
            right_copy(chip, 1 - core, sub, partner, t_send, t_recv).wait_recv()
        finish(piece(chip, 1 - core)[1])
    for sub in range(subs):
        for o in range(1, nchip):
            q = chip_peer(o)
            right_copy(q, core, sub, partner, r_send, r_recv).wait_recv()
            issue(right_copy(q, core, sub, partner, t_send, t_recv))
            if nrow == 1 and sub == subs - 1:
                finish(piece(q, core)[1])
    for o in range(1 if nrow == 1 else 0, nchip):
        q = chip_peer(o)
        for sub in range(subs):
            right_copy(q, 1 - core, sub, partner, t_send, t_recv).wait_recv()
        if nrow == 1:
            finish(piece(q, 1 - core)[1])
    if nrow > 1:
        for c in range(ncol):
            finish(pl.ds(c * pw, pw))

    others = pl.ds(0, spread - 1)
    copy(igs.at[others], igs.at[others], i_send, i_recv, dp=partner).wait_recv()

    for way in range(2):
        for s in range(nt):
            _, valid, b = origin(way, s)

            @pl.when(jnp.logical_and(valid, has_next(way)))
            def _():
                place = stack.at[token_rows(b), :]
                copy(place, place, act_send.at[way, s], act_recv.at[b, 0], tensor=z_peer(1)).wait_send()

    def sent(ref, send, recv):
        copy(ref, ref, send, recv, dp=partner).wait_send()

    if helped:
        @pl.when(at_end)
        def _():
            copy(warm.at[pl.ds(0, rank), warm_half(0)], warm.at[pl.ds(0, rank), warm_half(0)], f_send, f_recv.at[0], dp=partner).wait_send()

        @pl.when(inside)
        def _():
            warm_share(core).wait_send()
            told_copy().wait_send()

    sent(og.at[pl.ds(0, (nt - 1) * rows), :], o_send, o_recv)
    sent(ogp.at[others], g_send, g_recv)
    sent(wall.at[pl.ds(0, nt - 1)], w_send, w_recv.at[0])
    sent(igs.at[others], i_send, i_recv)
    sent(lefts.at[pl.ds(0, ndp - 1)], l_send, l_recv)
    sent(halves, h_send, h_recv.at[0])
    some = parts.at[:, pl.ds(0, nchip - 1)]
    sent(some, p_send, p_recv.at[0])
    sent(some, r_send, r_recv.at[0, 0])
    sent(halves, t_send, t_recv.at[0, 0])


def write_out(*refs):
    sems = refs[8]
    copies = []
    for i in range(4):
        src, dst = refs[i], refs[4 + i]
        count = PIECES if i == 0 else 2
        step = src.shape[0] // count
        for j in range(count):
            rows = pl.ds(j * step, step)
            copies.append(pltpu.make_async_copy(src.at[rows], dst.at[rows], sems.at[i, j]))
    for c in copies:
        c.start()
    for c in copies:
        c.wait()


def local(activations, out_grad, value_weight, error_feedback, warm_right):
    ndp, nt = lax.axis_size("dp"), lax.axis_size("tensor")
    layers = [[], [], [], []]
    for layer in range(activations.shape[0]):
        outs = one_layer(
            ndp, nt, activations[layer], out_grad[layer], value_weight[layer],
            error_feedback[layer, 0], warm_right[layer, 0].T,
        )
        for kept, out in zip(layers, outs):
            kept.append(out)
    residual, basis, factor, input_grad = [jnp.stack(kept) for kept in layers]
    return residual[:, None], basis.swapaxes(1, 2), factor.swapaxes(1, 2)[:, None], input_grad


def one_layer(ndp, nt, act, og, weight, error, warm):
    rows, width = act.shape
    tok, head = og.shape
    rank = warm.shape[0]
    spread = min(ndp, 8)
    ncol = min(ndp, width // 128)
    nrow = ndp // ncol
    nchip = ndp // 2
    ph, pw = rank // nrow, width // ncol
    subs = min(SUBS, ph // 8)
    dma = pltpu.SemaphoreType.DMA
    vmem = pl.BlockSpec(memory_space=pltpu.VMEM)
    shapes = (((head, width), BF16), ((rank, head), F32), ((rank, width), BF16), ((rows, width), BF16))
    results = pl.pallas_call(
        functools.partial(kernel, ndp, nt),
        out_shape=tuple(pltpu.VMEM(shape, dtype) for shape, dtype in shapes),
        in_specs=[pl.BlockSpec(memory_space=pltpu.HBM)] * 5,
        out_specs=(vmem,) * 4,
        scratch_shapes=[
            pltpu.VMEM((tok, head), BF16),
            pltpu.VMEM((tok + head, width), BF16),
            pltpu.VMEM((2 * rank, width), BF16),
            pltpu.VMEM((2 * rank, tok), F32),
            pltpu.VMEM((rank, tok), F32),
            pltpu.VMEM((nt, head, width // spread), BF16),
            pltpu.VMEM((spread, nt, rows, head), BF16),
            pltpu.VMEM((spread, rows, width // spread), BF16),
            pltpu.VMEM((head, width), F32),
            pltpu.VMEM((ndp, rank, head), F32),
            pltpu.VMEM((rank, width), F32),
            pltpu.VMEM((nchip, ph, pw), F32),
            pltpu.VMEM((subs, nchip, ph // subs, pw), F32),
            pltpu.VMEM((rank, width), F32),
            dma((6,)),
            dma((2, nt)), dma((nt, CHUNKS)),
            dma, dma((2,)), dma, dma,
            dma, dma, dma, dma,
            dma, dma((nt,)),
            dma, dma,
            dma, dma,
            dma, dma((nchip,)),
            dma, dma((subs,)),
            dma, dma((subs, nchip)),
            dma, dma((subs, nchip)),
        ],
        compiler_params=pltpu.CompilerParams(
            collective_id=0, has_side_effects=True, vmem_limit_bytes=62 * 1024 * 1024
        ),
    )(act, og, weight, error, warm)
    return pl.pallas_call(
        write_out,
        out_shape=tuple(jax.ShapeDtypeStruct(shape, dtype) for shape, dtype in shapes),
        in_specs=[vmem] * 4,
        out_specs=(pl.BlockSpec(memory_space=pltpu.HBM),) * 4,
        scratch_shapes=[dma((4, PIECES))],
        compiler_params=pltpu.CompilerParams(vmem_limit_bytes=16 * 1024 * 1024),
    )(*results)


def solution(mesh):
    return jax.shard_map(
        local,
        mesh=mesh,
        in_specs=(
            P(None, ("dp", "tensor"), None),
            P(None, "dp", "tensor"),
            P(None, "tensor", None),
            P(None, "dp", "tensor", None),
            P(None, "tensor", None, None),
        ),
        out_specs=(
            P(None, "dp", "tensor", None),
            P(None, "tensor", None),
            P(None, "tensor", None, None),
            P(None, ("dp", "tensor"), None),
        ),
        check_vma=False,
    )
```
